256 devices in a mesh: dp: 32 (over z_lo, x, y), tensor: 8 (over z_hi, core).
Axes of the slice: x: 4, y: 4, z: 8 (z_hi: 4, z_lo: 2; z = z_hi * 2 + z_lo), core: 2. Of those that a mesh axis runs over, the one named last changes fastest.
Arguments:
- hidden: bfloat16 [4096, 8192], P('dp')
- q_weight: float32 [8192, 4096], P(('dp', 'tensor')), may hold values from -0.0625 to 0.0625
- k_weight: float32 [8192, 1024], P(('dp', 'tensor')), may hold values from -0.0625 to 0.0625
- v_weight: float32 [8192, 1024], P(('dp', 'tensor')), may hold values from -0.0625 to 0.0625
- o_weight: float32 [8192, 4096], P(('dp', 'tensor')), may hold values from -0.09375 to 0.09375
- input_gain: float32 [8192], replicated, may hold values from 0.25 to 1.75
- post_gain: float32 [8192], replicated, may hold values from 0.25 to 1.75
- key_cache: bfloat16 [4096, 64, 8, 128], P('dp', None, 'tensor'), may hold values from -1000 to 1000
- value_cache: bfloat16 [4096, 64, 8, 128], P('dp', None, 'tensor'), may hold values from -6 to 6
- lengths: int32 [4096], P('dp'), may hold values from 1 to 64
Outputs:
- new_hidden: bfloat16 [4096, 8192], P('dp')
- normed: bfloat16 [4096, 8192], P('dp')
- fresh_token_keys: bfloat16 [4096, 8, 128], P('dp', 'tensor')
- new_values: bfloat16 [4096, 8, 128], P('dp', 'tensor')
The draws below stay inside these ranges and needn't reach their ends.
All inputs are finite; a program needn't handle non-finite values.
Results may differ from the reference program's by a relative error of at most 0.012.
The reference program's roundings to bfloat16 on the way count: a program that leaves them out, or rounds other values in their place, can miss the bound.
Values may be sent and summed in bfloat16 or wider, within the bound.
No kernel may reach another device: no remote copies, remote signals or barrier semaphores. Data moves between devices by JAX's collectives and lax.ppermute only.
A program may use at most 128 MiB of HBM per device.

```python
import math
import jax
import jax.numpy as jnp
from jax import lax

D = 8192
HEADS = 32
KV_HEADS = 8
HEAD_DIM = 128
CACHE = 64
QD = 4096
KD = 1024
GROUP = 4
BATCH = 4096


def draw_hidden(key, part):
    key_base, key_rows, key_column_slice = jax.random.split(key, 3)
    base = jax.random.normal(key_base, (BATCH, D), jnp.float32)
    row_scale = jnp.exp(jax.random.uniform(key_rows, (BATCH, 1), jnp.float32) * math.log(10.0))
    rising = jnp.exp(jnp.arange(D, dtype=jnp.float32)[None, :] / D * math.log(3.0))
    column_scale = jnp.exp(jax.random.uniform(key_column_slice, (1, D), jnp.float32) * math.log(10.0)) * rising
    return (0.03 * base * row_scale * column_scale).astype(jnp.bfloat16)


def draw_key_cache(key, part):
    key_base = jax.random.fold_in(key, 0)
    shape_full = (BATCH, CACHE, KV_HEADS, HEAD_DIM)
    base = jax.random.normal(key_base, shape_full, jnp.float32)
    return base.astype(jnp.bfloat16)


def touch_ends(entries, rng, low, top_value):
    longest = entries.shape.index(max(entries.shape))
    spots = []
    for shift in (0, 1):
        where = [jax.random.randint(jax.random.fold_in(rng, axis), (), 0, length) for axis, length in enumerate(entries.shape)]
        where[longest] = (where[longest] + shift) % entries.shape[longest]
        spots.append(tuple(where))
    return entries.at[spots[0]].set(low).at[spots[1]].set(top_value)


def block_scale(stream_key, shape, shards, least, top_value):
    loudness = 1.0
    for dim, shards_of in shards:
        heights = jax.random.uniform(jax.random.fold_in(jax.random.fold_in(stream_key, 6), dim), (shards_of,), jnp.float32, least / len(shards), top_value / len(shards))
        loudness = loudness * jnp.repeat(jnp.exp(heights), shape[dim] // shards_of).reshape((-1,) + (1,) * (len(shape) - 1 - dim))
    return loudness


def scatter_about(rng, dims, scale, reach, cuts=(), kind=jnp.bfloat16):
    values = jax.random.normal(rng, dims, jnp.float32) * scale
    if len(cuts) > 0:
        values = block_scale(rng, dims, cuts, -0.22, 0.18) * values
    return jnp.clip(values, min=-reach, max=reach).astype(kind)


def setup_inputs(seed: int = 0) -> dict:
    arg_keys = jax.random.split(jax.random.key(seed), 11)
    return {
        "hidden": draw_hidden(jax.random.fold_in(arg_keys[10], 71), 0),
        "q_weight": scatter_about(arg_keys[1], (D, QD), D ** -0.5, 0.0625, ((0, 256),), jnp.float32),
        "k_weight": scatter_about(arg_keys[2], (D, KD), D ** -0.5, 0.0625, ((0, 256),), jnp.float32),
        "v_weight": scatter_about(arg_keys[3], (D, KD), D ** -0.5, 0.0625, ((0, 256),), jnp.float32),
        "o_weight": scatter_about(arg_keys[4], (D, QD), QD ** -0.5, 0.09375, ((0, 256),), jnp.float32),
        "input_gain": jnp.clip(1.0 + 0.15 * jax.random.normal(arg_keys[5], (D,), jnp.float32), 0.25, 1.75),
        "post_gain": jnp.clip(1.0 + 0.15 * jax.random.normal(arg_keys[6], (D,), jnp.float32), 0.25, 1.75),
        "key_cache": draw_key_cache(jax.random.fold_in(arg_keys[10], 71), 0),
        "value_cache": scatter_about(arg_keys[8], (BATCH, CACHE, KV_HEADS, HEAD_DIM), 1.0, 6.0, ((0, 32), (2, 8))),
        "lengths": touch_ends(jax.random.randint(arg_keys[9], (BATCH,), 1, CACHE + 1), jax.random.fold_in(arg_keys[9], 1), 1, CACHE).astype(jnp.int32),
    }


epsilon = 1e-05
rope_base = 500000.0

def rms_gain(values, gain_vector):
    mean_square = lax.optimization_barrier(jnp.mean(values * values, axis=-1, keepdims=True))
    return values * lax.rsqrt(mean_square + epsilon) * gain_vector

def rotate(values, positions):
    half_dim = values.shape[-1] // 2
    index_row = jnp.arange(half_dim, dtype=jnp.float32)
    frequency = jnp.exp(-math.log(rope_base) * index_row / half_dim)
    angle = positions.astype(jnp.float32)[:, None, None] * frequency[None, None, :]
    first_half = values[..., :half_dim]
    second_half = values[..., half_dim:]
    return jnp.concatenate([first_half * jnp.cos(angle) - second_half * jnp.sin(angle), second_half * jnp.cos(angle) + first_half * jnp.sin(angle)], axis=-1)

def reference(hidden, q_weight, k_weight, v_weight, o_weight, input_gain, post_gain, key_cache, value_cache, lengths):
    w_query = q_weight.astype(jnp.bfloat16)
    w_key = k_weight.astype(jnp.bfloat16)
    value_matrix = v_weight.astype(jnp.bfloat16)
    w_out = o_weight.astype(jnp.bfloat16)
    row_count = hidden.shape[0]
    normal_in = rms_gain(hidden.astype(jnp.float32), input_gain).astype(jnp.bfloat16)
    query = jnp.dot(normal_in, w_query, preferred_element_type=jnp.float32)
    key_part = jnp.dot(normal_in, w_key, preferred_element_type=jnp.float32)
    value_part = jnp.dot(normal_in, value_matrix, preferred_element_type=jnp.float32)
    query_b = rotate(query.reshape(row_count, HEADS, HEAD_DIM), lengths).astype(jnp.bfloat16)
    fresh_token_keys = rotate(key_part.reshape(row_count, KV_HEADS, HEAD_DIM), lengths).astype(jnp.bfloat16)
    new_values = value_part.reshape(row_count, KV_HEADS, HEAD_DIM).astype(jnp.bfloat16)
    grouped_heads = query_b.astype(jnp.float32).reshape(row_count, KV_HEADS, GROUP, HEAD_DIM)
    reciprocal_root = 1.0 / math.sqrt(HEAD_DIM)
    scores = jnp.einsum('bkgd,blkd->bkgl', grouped_heads, key_cache.astype(jnp.float32)) * reciprocal_root
    self_token_score = jnp.einsum('lfxa,lfa->lfx', grouped_heads, fresh_token_keys.astype(jnp.float32)) * reciprocal_root
    visible = jnp.arange(CACHE, dtype=jnp.int32)[None, :] < lengths.astype(jnp.int32)[:, None]
    scores = jnp.where(visible[:, None, None, :], scores, -jnp.inf)
    largest = jnp.maximum(lax.optimization_barrier(jnp.max(scores, axis=-1)), self_token_score)
    kept_exp = jnp.exp(scores - largest[..., None])
    own_exp = jnp.exp(self_token_score - largest)
    softmax_divisor = lax.optimization_barrier(jnp.sum(kept_exp, axis=-1)) + own_exp
    weights_kept = (kept_exp / softmax_divisor[..., None]).astype(jnp.bfloat16)
    own_weight = (own_exp / softmax_divisor).astype(jnp.bfloat16)
    attended = jnp.einsum('bkgl,blkd->bkgd', weights_kept.astype(jnp.float32), value_cache.astype(jnp.float32))
    attended = attended + own_weight.astype(jnp.float32)[..., None] * new_values.astype(jnp.float32)[:, :, None, :]
    attended = attended.reshape(row_count, HEADS * HEAD_DIM).astype(jnp.bfloat16)
    mixed = jnp.dot(attended, w_out.T, preferred_element_type=jnp.float32)
    residual = hidden.astype(jnp.float32) + mixed
    new_hidden = residual.astype(jnp.bfloat16)
    normed = rms_gain(residual, post_gain).astype(jnp.bfloat16)
    return (new_hidden, normed, fresh_token_keys, new_values)
```

```python
import math

import jax
import jax.numpy as jnp
from jax import lax
from jax.experimental import pallas as pl
from jax.experimental.pallas import tpu as pltpu
from jax.sharding import Mesh
from jax.sharding import PartitionSpec as P

HEADS = 32
KV_HEADS = 8
HEAD_DIM = 128
ROWS = 128
D = 8192

epsilon = 1e-05
rope_base = 500000.0


bf16, f32 = jnp.bfloat16, jnp.float32
VM = pl.BlockSpec(memory_space=pltpu.VMEM)
SM = pl.BlockSpec(memory_space=pltpu.SMEM)


def shift(value, axis, size, step):
    return lax.ppermute(value, axis, [(i, (i + step) % size) for i in range(size)])


def at(array, index, dim=0):
    return lax.dynamic_index_in_dim(array, index, dim, keepdims=False)


def norm_kernel(idx, hid, gain, out, scale):
    zl, x, y, c = idx[0], idx[1], idx[2], idx[4]
    total = jnp.zeros((ROWS, 1), f32)
    for j in range(8):
        part = hid[:, j * 1024 : (j + 1) * 1024].astype(f32)
        total = total + jnp.sum(part * part, axis=-1, keepdims=True)
    scale[...] = jnp.broadcast_to(lax.rsqrt(total / D + epsilon), (ROWS, 128))
    for ys in range(4):
        for zs in range(2):
            for xs in range(4):
                col = ((zl ^ zs) * 4 + (x - xs) % 4) * 4 + (y + ys) % 4
                cols = pl.ds(pl.multiple_of(col * 256, 256), 256)
                g = gain[:, cols]
                for cr in range(2):
                    rows = pl.ds(pl.multiple_of((c ^ cr) * 64, 64), 64)
                    r = scale[rows, 0:1]
                    k = (zs * 4 + xs) * 256
                    value = hid[rows, cols].astype(f32) * r * g
                    out[ys, cr, :, k : k + 256] = value.astype(bf16)


def project_kernel(*refs):
    h0, hown, hpart = refs[0], refs[1:4], refs[4:7]
    w = refs[7:15]
    p0, p1, p2, p3 = refs[15:19]
    acc = refs[19]
    for k in range(8):
        ks = slice(k * 256, (k + 1) * 256)
        rows = [h0[0, :, ks], h0[1, :, ks]]
        for a, b in zip(hown, hpart):
            rows += [a[:, ks], b[:, ks]]
        part = jnp.dot(
            jnp.concatenate(rows, axis=0), w[k][...], preferred_element_type=f32
        )
        if k == 0:
            acc[...] = part
        elif k < 7:
            acc[...] += part
        else:
            part = acc[...] + part
            for s, p in enumerate((p0, p1, p2, p3)):
                p[...] = part[s * 128 : (s + 1) * 128].astype(p.dtype)


def out_kernel(*refs):
    idx = refs[0]
    own, part = refs[1:5], refs[5:9]
    a0, a1 = refs[9:13], refs[13:17]
    out, att, acc = refs[17:20]
    zh, c = idx[3], idx[4]
    for s in range(4):
        t = ((zh - s) % 4) * 2
        att[t + c] = own[s][...]
        att[t + 1 - c] = part[s][...]
    nt = (((1,), (1,)), ((), ()))
    halves = [
        jnp.concatenate([att[4 * h + j] for j in range(4)], axis=1) for h in range(2)
    ]
    for ys in range(4):
        lhs = a0[ys][...].reshape(256, 2048)
        got = lax.dot_general(lhs, halves[0], nt, preferred_element_type=f32)
        acc[:, ys] = got.reshape(4, 64, 128)
    for xs in range(4):
        lhs = a1[xs][...].reshape(256, 2048)
        got = lax.dot_general(lhs, halves[1], nt, preferred_element_type=f32)
        total = acc[xs] + got.reshape(4, 64, 128)
        out[xs] = total.astype(bf16)


def final_kernel(*refs):
    idx, own, part = refs[0], refs[1:5], refs[5:9]
    hid, gain = refs[9:11]
    new, normed = refs[11:13]
    pieces, res = refs[13:15]
    zl, x, y, zh, c = (idx[i] for i in range(5))
    for s in range(4):
        t = ((zh - s) % 4) * 2
        pieces[t + c] = own[s][...]
        pieces[t + 1 - c] = part[s][...]
    a = lax.broadcasted_iota(jnp.int32, (ROWS, ROWS), 0)
    b = lax.broadcasted_iota(jnp.int32, (ROWS, ROWS), 1)
    eye = jnp.where(a == b, 1.0, 0.0).astype(bf16)
    nt = (((1,), (1,)), ((), ()))
    total = jnp.zeros((ROWS, 1), f32)
    for xs in range(4):
        for ys in range(4):
            for zs in range(2):
                dp = ((zl ^ zs) * 4 + (x - xs) % 4) * 4 + (y - ys) % 4
                cols = pl.ds(pl.multiple_of(dp * 256, 256), 256)
                chunk = jnp.concatenate(
                    [pieces[t, xs, ys, zs * 32 : zs * 32 + 32] for t in range(8)],
                    axis=0,
                )
                mixed = lax.dot_general(eye, chunk, nt, preferred_element_type=f32)
                r = hid[:, cols].astype(f32) + mixed
                total = total + jnp.sum(r * r, axis=-1, keepdims=True)
                res[:, cols] = r
                new[:, cols] = r.astype(bf16)
    scale = lax.rsqrt(total / D + epsilon)
    for j in range(8):
        cols = slice(j * 1024, (j + 1) * 1024)
        normed[:, cols] = (res[:, cols] * scale * gain[:, cols]).astype(bf16)


def rotate(values, positions):
    half_dim = values.shape[-1] // 2
    index_row = jnp.arange(half_dim, dtype=f32)
    frequency = jnp.exp(-math.log(rope_base) * index_row / half_dim)
    angle = positions.astype(f32)[:, None, None] * frequency[None, None, :]
    first_half = values[..., :half_dim]
    second_half = values[..., half_dim:]
    return jnp.concatenate(
        [
            first_half * jnp.cos(angle) - second_half * jnp.sin(angle),
            second_half * jnp.cos(angle) + first_half * jnp.sin(angle),
        ],
        axis=-1,
    )


def attend(query_b, fresh_token_keys, new_values, key_cache, value_cache, lengths):
    row_count, kv_count = (fresh_token_keys.shape[0], fresh_token_keys.shape[1])
    grouped_heads = query_b.reshape(row_count, kv_count, -1, HEAD_DIM)
    reciprocal_root = 1.0 / math.sqrt(HEAD_DIM)
    scores = (
        jnp.einsum("bkgd,blkd->bkgl", grouped_heads, key_cache, preferred_element_type=f32)
        * reciprocal_root
    )
    self_token_score = (
        jnp.einsum("lfxa,lfa->lfx", grouped_heads, fresh_token_keys, preferred_element_type=f32)
        * reciprocal_root
    )
    visible = jnp.arange(key_cache.shape[1], dtype=jnp.int32)[None, :] < lengths[:, None]
    scores = jnp.where(visible[:, None, None, :], scores, -jnp.inf)
    largest = jnp.maximum(jnp.max(scores, axis=-1), self_token_score)
    kept_exp = jnp.exp(scores - largest[..., None])
    own_exp = jnp.exp(self_token_score - largest)
    softmax_divisor = jnp.sum(kept_exp, axis=-1) + own_exp
    weights_kept = (kept_exp / softmax_divisor[..., None]).astype(bf16)
    own_weight = (own_exp / softmax_divisor).astype(bf16)
    attended = jnp.einsum(
        "bkgl,blkd->bkgd", weights_kept, value_cache, preferred_element_type=f32
    )
    attended = attended + own_weight.astype(f32)[..., None] * new_values.astype(f32)[:, :, None, :]
    return attended.reshape(row_count, -1).astype(bf16)


def shards(hidden, q_weight, k_weight, v_weight, o_weight, input_gain, post_gain, key_cache, value_cache, lengths):
    zl, x, y, zh, c = (lax.axis_index(a) for a in ("zl", "x", "y", "zh", "c"))
    idx = jnp.stack([zl, x, y, zh, c]).astype(jnp.int32)
    sds = jax.ShapeDtypeStruct

    cut = jnp.concatenate(
        [
            q_weight.reshape(32, 4, 2, 512),
            k_weight.reshape(32, 4, 2, 128),
            v_weight.reshape(32, 4, 2, 128),
        ],
        axis=-1,
    ).astype(bf16).transpose(1, 2, 0, 3)
    mine, others = at(cut, c, 1), at(cut, 1 - c, 1)
    got = shift(others, "c", 2, 1)
    both = jnp.concatenate(
        [jnp.where(c == 0, mine, got), jnp.where(c == 0, got, mine)], axis=1
    )
    block = jnp.zeros((4, 64, 768), bf16)
    for s in range(4):
        piece = at(both, (zh + s) % 4)
        if s:
            piece = shift(piece, "zh", 4, s)
        block = lax.dynamic_update_index_in_dim(block, piece, (zh - s) % 4, 0)
    block = block.reshape(256, 768)
    across = shift(block, "zl", 2, 1)
    weights = [b if s == 0 else shift(b, "x", 4, s) for b in (block, across) for s in range(4)]

    nin = pl.pallas_call(
        norm_kernel,
        out_shape=sds((4, 2, 64, 2048), bf16),
        in_specs=[SM, VM, VM],
        out_specs=VM,
        scratch_shapes=[pltpu.VMEM((ROWS, 128), f32)],
    )(idx, hidden, input_gain.reshape(1, D))
    hown = [shift(nin[s, 0], "y", 4, s) for s in (1, 2, 3)]
    hpart = [shift(h, "c", 2, 1) for h in hown]

    parts = pl.pallas_call(
        project_kernel,
        out_shape=[sds((ROWS, 768), f32)] * 4,
        in_specs=[VM] * 15,
        out_specs=[VM] * 4,
        scratch_shapes=[pltpu.VMEM((512, 768), f32)],
    )(nin[0], *hown, *hpart, *weights)
    qkv = parts[0]
    for s in (1, 2, 3):
        qkv = qkv + shift(parts[s], "y", 4, -s)
    qkv = jnp.where(c == 0, qkv, jnp.concatenate([qkv[64:], qkv[:64]], axis=0))

    query, key_part, value_part = qkv[:, :512], qkv[:, 512:640], qkv[:, 640:]
    query_b = rotate(query.reshape(ROWS, 4, HEAD_DIM), lengths).astype(bf16)
    fresh_token_keys = rotate(key_part.reshape(ROWS, 1, HEAD_DIM), lengths).astype(bf16)
    new_values = value_part.reshape(ROWS, 1, HEAD_DIM).astype(bf16)
    attended = attend(query_b, fresh_token_keys, new_values, key_cache, value_cache, lengths)

    ob = o_weight.astype(bf16)
    both_o = jnp.stack([ob, shift(ob, "zl", 2, 1)])
    h0, h1 = both_o[..., :2048], both_o[..., 2048:]
    s0 = jnp.stack([h0 if s == 0 else shift(h0, "x", 4, s) for s in range(4)])
    s1 = jnp.stack([h1 if s == 0 else shift(h1, "y", 4, s) for s in range(4)])
    a0 = [s0 if s == 0 else shift(s0, "y", 4, s) for s in range(4)]
    a1 = [s1 if s == 0 else shift(s1, "x", 4, s) for s in range(4)]

    att_own = [attended if s == 0 else shift(attended, "zh", 4, s) for s in range(4)]
    att_part = [shift(a, "c", 2, 1) for a in att_own]
    mixed_t = pl.pallas_call(
        out_kernel,
        out_shape=sds((4, 4, 64, ROWS), bf16),
        in_specs=[SM] + [VM] * 16,
        out_specs=VM,
        scratch_shapes=[pltpu.VMEM((8, ROWS, 512), bf16), pltpu.VMEM((4, 4, 64, ROWS), f32)],
    )(idx, *att_own, *att_part, *a0, *a1)
    m_own = [mixed_t if s == 0 else shift(mixed_t, "zh", 4, s) for s in range(4)]
    m_part = [shift(m, "c", 2, 1) for m in m_own]
    new_hidden, normed = pl.pallas_call(
        final_kernel,
        out_shape=[sds((ROWS, D), bf16)] * 2,
        in_specs=[SM] + [VM] * 10,
        out_specs=[VM] * 2,
        scratch_shapes=[pltpu.VMEM((8, 4, 4, 64, ROWS), bf16), pltpu.VMEM((ROWS, D), f32)],
    )(idx, *m_own, *m_part, hidden, post_gain.reshape(1, D))
    return (new_hidden, normed, fresh_token_keys, new_values)


def solution(mesh):
    torus = Mesh(mesh.devices.reshape(2, 4, 4, 4, 2), ("zl", "x", "y", "zh", "c"))
    dp, tensor = ("zl", "x", "y"), ("zh", "c")
    in_specs = (
        P(dp, None),
        P(dp + tensor, None),
        P(dp + tensor, None),
        P(dp + tensor, None),
        P(dp + tensor, None),
        P(),
        P(),
        P(dp, None, tensor, None),
        P(dp, None, tensor, None),
        P(dp),
    )
    out_specs = (P(dp, None), P(dp, None), P(dp, tensor, None), P(dp, tensor, None))
    return jax.shard_map(shards, mesh=torus, in_specs=in_specs, out_specs=out_specs, check_vma=False)
```

```python
import math

import jax
import jax.numpy as jnp
from jax import lax
from jax.experimental import pallas as pl
from jax.experimental.pallas import tpu as pltpu
from jax.sharding import Mesh
from jax.sharding import PartitionSpec as P


HEAD_DIM = 128
ROWS = 128
D = 8192
CUT = 1024

epsilon = 1e-05
rope_base = 500000.0


bf16, f32 = jnp.bfloat16, jnp.float32
VM = pl.BlockSpec(memory_space=pltpu.VMEM)
SM = pl.BlockSpec(memory_space=pltpu.SMEM)


def shift(value, axis, size, step):
    return lax.ppermute(value, axis, [(i, (i + step) % size) for i in range(size)])


def cut_kernel(q, k, v, out):
    for t in range(8):
        out[t, :, 0:512] = q[:, t * 512 : t * 512 + 512].astype(bf16)
        out[t, :, 512:640] = k[:, t * 128 : t * 128 + 128].astype(bf16)
        out[t, :, 640:768] = v[:, t * 128 : t * 128 + 128].astype(bf16)


def norm_kernel(idx, hid, gain, own, send1, send2, send3, scale):
    zl, x, y, c = idx[0], idx[1], idx[2], idx[4]

    def add(j, total):
        part = hid[:, pl.ds(pl.multiple_of(j * 1024, 1024), 1024)].astype(f32)
        return total + jnp.sum(part * part, axis=-1, keepdims=True)

    total = lax.fori_loop(0, 8, add, jnp.zeros((ROWS, 1), f32))
    scale[...] = jnp.broadcast_to(lax.rsqrt(total / D + epsilon), (ROWS, 128))

    def step(j, carry):
        zs, xs = j // 4, j % 4
        there = ((zl ^ zs) * 4 + (x + 4 - xs) % 4) * 4
        to = pl.ds(pl.multiple_of(j * 256, 256), 256)
        for ys, out in ((1, send1), (2, send2), (3, send3), (0, own)):
            cols = pl.ds(pl.multiple_of((there + (y + ys) % 4) * 256, 256), 256)
            g = gain[:, cols]
            for cr in range(1 if ys else 2):
                rows = pl.ds(pl.multiple_of((c ^ cr) * 64, 64), 64)
                value = hid[rows, cols].astype(f32) * scale[rows, 0:1] * g
                if ys:
                    out[:, to] = value.astype(bf16)
                else:
                    out[cr, :, to] = value.astype(bf16)
        return carry

    lax.fori_loop(0, 8, step, 0)


def left_rows(h0, hown, hpart, ks):
    rows = [h0[0, :, ks], h0[1, :, ks]]
    for s in range(3):
        rows += [hown[s][:, ks], hpart[s, :, ks]]
    return jnp.concatenate(rows, axis=0)


def first_kernel(h0, ha, hb, hc, hpart, w0, w1, w3, v0, acc):
    def step(n, carry):
        cols = pl.ds(pl.multiple_of(n * 256, 256), 256)
        part = jnp.zeros((512, 256), f32)
        for k, w in ((0, w0), (1, w1), (3, w3), (4, v0)):
            lhs = left_rows(h0, (ha, hb, hc), hpart, slice(k * 256, k * 256 + 256))
            part = part + jnp.dot(lhs, w[:, cols], preferred_element_type=f32)
        acc[:, cols] = part
        return carry

    lax.fori_loop(0, 3, step, 0)


def second_kernel(h0, ha, hb, hc, hpart, v1, v3, wa, wb, va, vb, acc, p0, p1, p2, p3):
    def step(n, carry):
        cols = pl.ds(pl.multiple_of(n * 256, 256), 256)
        part = acc[:, cols]
        for k, w in ((5, (v1,)), (7, (v3,)), (2, (wa, wb)), (6, (va, vb))):
            lhs = left_rows(h0, (ha, hb, hc), hpart, slice(k * 256, k * 256 + 256))
            rhs = jnp.concatenate([r[:, cols] for r in w], axis=0)
            part = part + jnp.dot(lhs, rhs, preferred_element_type=f32)
        for s, p in enumerate((p0, p1, p2, p3)):
            p[:, cols] = part[s * 128 : (s + 1) * 128].astype(p.dtype)
        return carry

    lax.fori_loop(0, 3, step, 0)


def attend_kernel(idx, p0, r1, r2, r3, cos, sin, lengths, keys, vals, att, fresh, newv, qkv, qs, fs, vs, sc, out):
    c = idx[4]
    total = p0[...] + r1[...].astype(f32) + r2[...].astype(f32) + r3[...].astype(f32)
    qkv[pl.ds(pl.multiple_of(c * 64, 64), 64)] = total[:64]
    qkv[pl.ds(pl.multiple_of(64 - c * 64, 64), 64)] = total[64:]

    def turn(v):
        return (v * cos[...] + pltpu.roll(v, 64, 1) * sin[...]).astype(bf16)

    fk = turn(qkv[:, 512:640])
    nv = qkv[:, 640:768].astype(bf16)
    fresh[...] = fk
    newv[...] = nv
    fs[...] = fk.astype(f32).reshape(16, 8, 128)
    vs[...] = nv.astype(f32).reshape(16, 8, 128)
    for h in range(4):
        qs[:, h] = turn(qkv[:, h * 128 : h * 128 + 128]).astype(f32).reshape(16, 8, 128)
    root = 1.0 / math.sqrt(HEAD_DIM)

    def score(g, carry):
        q = qs[g].reshape(32, 128).astype(bf16)
        k = keys[pl.ds(g * 8, 8)].reshape(512, 128)
        sc[g] = lax.dot_general(q, k, (((1,), (1,)), ((), ())), preferred_element_type=f32)
        return carry

    lax.fori_loop(0, 16, score, 0, unroll=4)
    col = lax.broadcasted_iota(jnp.int32, (4, 8, 512), 2)
    row = lax.broadcasted_iota(jnp.int32, (4, 8, 512), 1)
    mine = (col // 64) == row
    pos = (col % 64).astype(f32)

    def weigh(g, carry):
        s = sc[g].reshape(4, 8, 512) * root
        here = lengths[pl.ds(pl.multiple_of(g * 8, 8), 8), 0:1]
        keep = jnp.logical_and(mine, pos < here[None])
        s = jnp.where(keep, s, -jnp.inf)
        own = jnp.sum(qs[g] * fs[g][None], axis=-1, keepdims=True) * root
        top = jnp.maximum(jnp.max(s, axis=-1, keepdims=True), own)
        e = jnp.exp(s - top)
        eo = jnp.exp(own - top)
        div = jnp.sum(e, axis=-1, keepdims=True) + eo
        w = (e / div).astype(bf16).reshape(32, 512)
        wo = (eo / div).astype(bf16).astype(f32)
        v = vals[pl.ds(g * 8, 8)].reshape(512, 128)
        o = jnp.dot(w, v, preferred_element_type=f32).reshape(4, 8, 128) + wo * vs[g][None]
        for h in range(4):
            out[g, :, h * 128 : h * 128 + 128] = o[h]
        return carry

    lax.fori_loop(0, 16, weigh, 0, unroll=4)
    att[...] = out[...].reshape(ROWS, 512).astype(bf16)


def place(zh, c, own, part, into):
    for s in range(4):
        t = ((zh + 4 - s) % 4) * 2
        into[t + c] = own[s]
        into[t + 1 - c] = part[s]


def rows_kernel(idx, w, mine, other):
    zl = idx[0]
    for q in range(2):
        to = slice(q * 1024, q * 1024 + 1024)
        for out, z in ((mine, zl), (other, 1 - zl)):
            cols = pl.ds(pl.multiple_of(q * 2048 + z * 1024, 1024), 1024)
            out[:, to] = w[:, cols].astype(bf16)


def halves_kernel(mine, got, e0, e1):
    for z, w in enumerate((mine, got)):
        e0[z] = w[:, :CUT]
        e1[z] = w[:, CUT:]


def out_kernel(*refs):
    idx = refs[0]
    own, three, two = refs[1:5], refs[5], refs[6]
    part = (three[0], three[1], two[...], three[2])
    ya, xa = refs[7:11], refs[11:15]
    keep, send, att, acc0, acc1 = refs[15:20]
    zl, zh, c = idx[0], idx[3], idx[4]
    for s in range(4):
        k = (zh + 4 - s) % 4
        rows = pl.ds(pl.multiple_of(k % 2 * ROWS, ROWS), ROWS)
        att[k // 2 * 2 + c, rows] = own[s][...]
        att[k // 2 * 2 + 1 - c, rows] = part[s]
    nt = (((1,), (1,)), ((), ()))

    def add(a, acc, first):
        def step(t, carry):
            for u in range(2):
                cols = pl.ds(pl.multiple_of(t * 512 + u * 256, 256), 256)
                lhs = jnp.concatenate([r[:, :, :, cols].reshape(-1, 256) for r in a], axis=0)
                rhs = att[first + t][:, u * 256 : u * 256 + 256]
                acc[...] += lax.dot_general(lhs, rhs, nt, preferred_element_type=f32)
            return carry

        return step

    acc0[...] = jnp.zeros((1024, 256), f32)
    acc1[...] = jnp.zeros((1024, 256), f32)
    for a, acc, first, last in ((ya, acc0, 0, CUT), (xa, acc1, CUT, 2048)):
        lax.fori_loop(0, (last - first) // 512, add(a, acc, first // 512), 0)
    here = pl.ds(pl.multiple_of(zl * ROWS, ROWS), ROWS)
    there = pl.ds(pl.multiple_of(ROWS - zl * ROWS, ROWS), ROWS)
    for xs in range(4):
        for ys in range(4):
            i, j = (ys * 4 + xs) * 64, (xs * 4 + ys) * 64
            keep[xs, ys] = acc0[i : i + 64, here] + acc1[j : j + 64, here]
            total = (acc0[i : i + 64, there] + acc1[j : j + 64, there]).astype(bf16)
            send[xs, ys, 0:32] = total[32:]
            send[xs, ys, 32:64] = total[:32]


def add_kernel(keep, got, out):
    for xs in range(4):
        out[xs] = (keep[xs] + got[xs].astype(f32)).astype(bf16)


def final_kernel(*refs):
    idx = refs[0]
    own = [r[...] for r in refs[1:5]]
    part = [refs[5][0], refs[5][1], refs[6][...], refs[5][2]]
    hid, gain, new, normed, pieces, res = refs[7:13]
    zl, x, y = idx[0], idx[1], idx[2]
    place(idx[3], idx[4], own, part, pieces)
    a = lax.broadcasted_iota(jnp.int32, (ROWS, ROWS), 0)
    b = lax.broadcasted_iota(jnp.int32, (ROWS, ROWS), 1)
    eye = jnp.where(a == b, 1.0, 0.0).astype(bf16)
    nt = (((1,), (1,)), ((), ()))

    def step(j, total):
        xs, ys = j // 4, j % 4
        for zs in range(2):
            dp = ((zl ^ zs) * 4 + (x + 4 - xs) % 4) * 4 + (y + 4 - ys) % 4
            cols = pl.ds(pl.multiple_of(dp * 256, 256), 256)
            chunk = jnp.concatenate(
                [pieces[t, xs, ys, zs * 32 : zs * 32 + 32] for t in range(8)], axis=0
            )
            mixed = lax.dot_general(eye, chunk, nt, preferred_element_type=f32)
            r = hid[:, cols].astype(f32) + mixed
            total = total + r * r
            res[:, cols] = r
            new[:, cols] = r.astype(bf16)
        return total

    total = lax.fori_loop(0, 16, step, jnp.zeros((ROWS, 256), f32), unroll=2)
    scale = lax.rsqrt(jnp.sum(total, axis=-1, keepdims=True) / D + epsilon)

    def finish(j, carry):
        cols = pl.ds(pl.multiple_of(j * 1024, 1024), 1024)
        normed[:, cols] = (res[:, cols] * scale * gain[:, cols]).astype(bf16)
        return carry

    lax.fori_loop(0, 8, finish, 0)


def call(kernel, outs, *args, scratch=(), limit=16, near=True):
    def scalars(a):
        return a.dtype == jnp.int32 and a.ndim == 1

    return pl.pallas_call(
        kernel,
        out_shape=outs,
        in_specs=[SM if scalars(a) else VM for a in args],
        out_specs=jax.tree.map(lambda _: VM, outs),
        scratch_shapes=[pltpu.VMEM(*x) for x in scratch],
        compiler_params=pltpu.CompilerParams(vmem_limit_bytes=limit << 20),
    )(*[a if scalars(a) or not near else pltpu.with_memory_space_constraint(a, pltpu.VMEM) for a in args])


def fetch_kernel(keys, vals, keys_out, vals_out, sems):
    first = pltpu.make_async_copy(keys, keys_out, sems.at[0])
    second = pltpu.make_async_copy(vals, vals_out, sems.at[1])
    first.start()
    second.start()
    first.wait()
    second.wait()


def fetch(keys, vals):
    cache = pltpu.VMEM((ROWS, 64, HEAD_DIM), bf16)
    hbm = pl.BlockSpec(memory_space=pl.ANY)
    return pl.pallas_call(
        fetch_kernel,
        out_shape=[cache, cache],
        in_specs=[hbm, hbm],
        out_specs=[VM, VM],
        scratch_shapes=[pltpu.SemaphoreType.DMA((2,))],
        compiler_params=pltpu.CompilerParams(vmem_limit_bytes=1 << 20),
        name="fetch",
    )(keys, vals)


def body(hidden, q_weight, k_weight, v_weight, o_weight, input_gain, post_gain, key_cache, value_cache, lengths):
    zl, x, y, zh, c = (lax.axis_index(a) for a in ("zl", "x", "y", "zh", "c"))
    idx = idx0 = jnp.stack([zl, x, y, zh, c]).astype(jnp.int32)
    sds, vm = jax.ShapeDtypeStruct, pltpu.VMEM

    def move(value, axis, step):
        return shift(value, axis, 2 if axis in ("zl", "c") else 4, step)

    cut = call(cut_kernel, vm((8, 32, 768), bf16), q_weight, k_weight, v_weight, near=False, limit=60)
    block = lax.all_to_all(cut, ("zh", "c"), split_axis=0, concat_axis=0, tiled=True)
    block = block.reshape(256, 768)
    across = move(block, "zl", 1)
    w1, w3 = move(block, "x", 1), move(block, "x", 3)
    v1, v3 = move(across, "x", 1), move(across, "x", 3)
    wa, wb = move(w1[:128], "x", 1), move(w3[128:], "x", 3)
    va, vb = move(v1[:128], "x", 1), move(v3[128:], "x", 3)

    half = pltpu.HBM((64, 2048), bf16)
    h0, *hs = call(
        norm_kernel,
        [pltpu.HBM((2, 64, 2048), bf16), half, half, half],
        idx, hidden, input_gain.reshape(1, D),
        scratch=[((ROWS, 128), f32)],
    )
    hown = [move(hs[s - 1], "y", s) for s in (1, 2, 3)]
    hpart = move(jnp.stack(hown), "c", 1)

    acc = call(first_kernel, vm((512, 768), f32), h0, *hown, hpart, block, w1, w3, across, limit=8)
    full, short = vm((ROWS, 768), f32), vm((ROWS, 768), bf16)
    parts = call(second_kernel, [full, short, short, short], h0, *hown, hpart, v1, v3, wa, wb, va, vb, acc, limit=8)
    back = [move(parts[s], "y", -s) for s in (1, 2, 3)]

    index_row = jnp.arange(64, dtype=f32)
    frequency = jnp.exp(-math.log(rope_base) * index_row / 64)
    angle = lengths.astype(f32)[:, None] * frequency[None, :]
    cos, sin = jnp.cos(angle), jnp.sin(angle)
    head = sds((ROWS, 128), bf16)
    attended, fresh, newv = call(
        attend_kernel,
        [vm((ROWS, 512), bf16), head, head],
        idx, parts[0], *back,
        jnp.concatenate([cos, cos], axis=1),
        jnp.concatenate([-sin, sin], axis=1),
        jnp.broadcast_to(lengths.astype(f32)[:, None], (ROWS, 128)),
        *fetch(key_cache.reshape(ROWS, 64, 128), value_cache.reshape(ROWS, 64, 128)),
        scratch=[
            ((ROWS, 768), f32),
            ((16, 4, 8, 128), f32),
            ((16, 8, 128), f32),
            ((16, 8, 128), f32),
            ((16, 32, 512), f32),
            ((16, 8, 512), f32),
        ],
    )

    shard = vm((32, 2048), bf16)
    mine_o, other_o = call(rows_kernel, [shard] * 2, idx0, o_weight, near=False, limit=60)
    e0, e1 = call(
        halves_kernel,
        [vm((2, 32, CUT), bf16), vm((2, 32, 2048 - CUT), bf16)],
        mine_o, move(other_o, "zl", 1),
    )
    around = [e0] + [move(e0, "x", s) for s in (1, 2, 3)]
    s0 = jnp.stack(around)
    s1 = jnp.stack([e1] + [move(e1, "y", s) for s in (1, 2, 3)])
    rows_y = [s0] + [move(s0, "y", s) for s in (1, 2, 3)]
    rows_x = [s1] + [move(s1, "x", s) for s in (1, 2, 3)]

    def deal_heads(value, turn):
        pairs = []
        for z in range(8):
            to = z // 2 % 2 * 4 + (z % 2 + z // 4 * 2 + turn) % 4
            pairs.append((z % 2 * 4 + z // 2, to))
        return lax.ppermute(value, ("zl", "zh"), pairs)

    def spread(own):
        first = move(jnp.stack([own[0], own[1], own[3]]), "c", 1)
        return own + [first, move(own[2], "c", 1)]

    heads = spread([deal_heads(attended, s) for s in range(4)])
    tile = (4, 4, 64, ROWS)
    keep, send = call(
        out_kernel,
        [vm(tile, f32), vm(tile, bf16)],
        idx, *heads, *rows_y, *rows_x,
        scratch=[((4, 256, 512), bf16), ((1024, 256), f32), ((1024, 256), f32)],
    )
    mixed_t = call(add_kernel, vm(tile, bf16), keep, move(send, "zl", 1), limit=4)
    pieces = spread([mixed_t] + [move(mixed_t, "zh", s) for s in (1, 2, 3)])
    new_hidden, normed = call(
        final_kernel,
        [sds((ROWS, D), bf16)] * 2,
        idx, *pieces, hidden, post_gain.reshape(1, D),
        scratch=[((8, 4, 4, 64, ROWS), bf16), ((ROWS, D), f32)],
    )
    return (new_hidden, normed, fresh.reshape(ROWS, 1, 128), newv.reshape(ROWS, 1, 128))


def solution(mesh):
    torus = Mesh(mesh.devices.reshape(2, 4, 4, 4, 2), ("zl", "x", "y", "zh", "c"))
    dp, tensor = ("zl", "x", "y"), ("zh", "c")
    in_specs = (
        P(dp, None),
        P(dp + tensor, None),
        P(dp + tensor, None),
        P(dp + tensor, None),
        P(dp + tensor, None),
        P(),
        P(),
        P(dp, None, tensor, None),
        P(dp, None, tensor, None),
        P(dp),
    )
    out_specs = (P(dp, None), P(dp, None), P(dp, tensor, None), P(dp, tensor, None))
    return jax.shard_map(body, mesh=torus, in_specs=in_specs, out_specs=out_specs, check_vma=False)
```

```python
import math

import jax
import jax.numpy as jnp
from jax import lax
from jax.experimental import pallas as pl
from jax.experimental.pallas import tpu as pltpu
from jax.sharding import Mesh
from jax.sharding import PartitionSpec as P


HEAD_DIM = 128
ROWS = 128
D = 8192
CUT = 1024

epsilon = 1e-05
rope_base = 500000.0


bf16, f32 = jnp.bfloat16, jnp.float32
VM = pl.BlockSpec(memory_space=pltpu.VMEM)
SM = pl.BlockSpec(memory_space=pltpu.SMEM)


def shift(value, axis, size, step):
    return lax.ppermute(value, axis, [(i, (i + step) % size) for i in range(size)])


def cut_kernel(q, k, v, out):
    for t in range(8):
        out[t, :, 0:512] = q[:, t * 512 : t * 512 + 512].astype(bf16)
        out[t, :, 512:640] = k[:, t * 128 : t * 128 + 128].astype(bf16)
        out[t, :, 640:768] = v[:, t * 128 : t * 128 + 128].astype(bf16)


def norm_kernel(idx, hid, gain, own, send1, send2, send3, scale):
    zl, x, y, c = idx[0], idx[1], idx[2], idx[4]

    def add(j, total):
        part = hid[:, pl.ds(pl.multiple_of(j * 1024, 1024), 1024)].astype(f32)
        return total + jnp.sum(part * part, axis=-1, keepdims=True)

    total = lax.fori_loop(0, 8, add, jnp.zeros((ROWS, 1), f32))
    scale[...] = jnp.broadcast_to(lax.rsqrt(total / D + epsilon), (ROWS, 128))

    def step(j, carry):
        zs, xs = j // 4, j % 4
        there = ((zl ^ zs) * 4 + (x + 4 - xs) % 4) * 4
        to = pl.ds(pl.multiple_of(j * 256, 256), 256)
        for ys, out in ((1, send1), (2, send2), (3, send3), (0, own)):
            cols = pl.ds(pl.multiple_of((there + (y + ys) % 4) * 256, 256), 256)
            g = gain[:, cols]
            for cr in range(1 if ys else 2):
                rows = pl.ds(pl.multiple_of((c ^ cr) * 64, 64), 64)
                value = hid[rows, cols].astype(f32) * scale[rows, 0:1] * g
                if ys:
                    out[:, to] = value.astype(bf16)
                else:
                    out[cr, :, to] = value.astype(bf16)
        return carry

    lax.fori_loop(0, 8, step, 0)


def left_rows(h0, hown, hpart, ks):
    rows = [h0[0, :, ks], h0[1, :, ks]]
    for s in range(3):
        rows += [hown[s][:, ks], hpart[s, :, ks]]
    return jnp.concatenate(rows, axis=0)


def first_kernel(h0, ha, hb, hc, hpart, w0, w1, w3, v0, acc):
    def step(n, carry):
        cols = pl.ds(pl.multiple_of(n * 256, 256), 256)
        part = jnp.zeros((512, 256), f32)
        for k, w in ((0, w0), (1, w1), (3, w3), (4, v0)):
            lhs = left_rows(h0, (ha, hb, hc), hpart, slice(k * 256, k * 256 + 256))
            part = part + jnp.dot(lhs, w[:, cols], preferred_element_type=f32)
        acc[:, cols] = part
        return carry

    lax.fori_loop(0, 3, step, 0)


def second_kernel(h0, ha, hb, hc, hpart, v1, v3, wa, wb, va, vb, acc, p0, p1, p2, p3):
    def step(n, carry):
        cols = pl.ds(pl.multiple_of(n * 256, 256), 256)
        part = acc[:, cols]
        for k, w in ((5, (v1,)), (7, (v3,)), (2, (wa, wb)), (6, (va, vb))):
            lhs = left_rows(h0, (ha, hb, hc), hpart, slice(k * 256, k * 256 + 256))
            rhs = jnp.concatenate([r[:, cols] for r in w], axis=0)
            part = part + jnp.dot(lhs, rhs, preferred_element_type=f32)
        for s, p in enumerate((p0, p1, p2, p3)):
            p[:, cols] = part[s * 128 : (s + 1) * 128].astype(p.dtype)
        return carry

    lax.fori_loop(0, 3, step, 0)


def attend_kernel(idx, p0, r1, r2, r3, cos, sin, lengths, keys, vals, att, fresh, newv, qkv, qs, fs, vs, sc, out):
    c = idx[4]
    total = p0[...] + r1[...].astype(f32) + r2[...].astype(f32) + r3[...].astype(f32)
    qkv[pl.ds(pl.multiple_of(c * 64, 64), 64)] = total[:64]
    qkv[pl.ds(pl.multiple_of(64 - c * 64, 64), 64)] = total[64:]

    def turn(v):
        return (v * cos[...] + pltpu.roll(v, 64, 1) * sin[...]).astype(bf16)

    fk = turn(qkv[:, 512:640])
    nv = qkv[:, 640:768].astype(bf16)
    fresh[...] = fk
    newv[...] = nv
    fs[...] = fk.astype(f32).reshape(16, 8, 128)
    vs[...] = nv.astype(f32).reshape(16, 8, 128)
    for h in range(4):
        qs[:, h] = turn(qkv[:, h * 128 : h * 128 + 128]).astype(f32).reshape(16, 8, 128)
    root = 1.0 / math.sqrt(HEAD_DIM)

    def score(g, carry):
        q = qs[g].reshape(32, 128).astype(bf16)
        k = keys[pl.ds(g * 8, 8)].reshape(512, 128)
        sc[g] = lax.dot_general(q, k, (((1,), (1,)), ((), ())), preferred_element_type=f32)
        return carry

    lax.fori_loop(0, 16, score, 0, unroll=4)
    col = lax.broadcasted_iota(jnp.int32, (4, 8, 512), 2)
    row = lax.broadcasted_iota(jnp.int32, (4, 8, 512), 1)
    mine = (col // 64) == row
    pos = (col % 64).astype(f32)

    def weigh(g, carry):
        s = sc[g].reshape(4, 8, 512) * root
        here = lengths[pl.ds(pl.multiple_of(g * 8, 8), 8), 0:1]
        keep = jnp.logical_and(mine, pos < here[None])
        s = jnp.where(keep, s, -jnp.inf)
        own = jnp.sum(qs[g] * fs[g][None], axis=-1, keepdims=True) * root
        top = jnp.maximum(jnp.max(s, axis=-1, keepdims=True), own)
        e = jnp.exp(s - top)
        eo = jnp.exp(own - top)
        div = jnp.sum(e, axis=-1, keepdims=True) + eo
        w = (e / div).astype(bf16).reshape(32, 512)
        wo = (eo / div).astype(bf16).astype(f32)
        v = vals[pl.ds(g * 8, 8)].reshape(512, 128)
        o = jnp.dot(w, v, preferred_element_type=f32).reshape(4, 8, 128) + wo * vs[g][None]
        for h in range(4):
            out[g, :, h * 128 : h * 128 + 128] = o[h]
        return carry

    lax.fori_loop(0, 16, weigh, 0, unroll=4)
    att[...] = out[...].reshape(ROWS, 512).astype(bf16)


def rows_kernel(idx, w, mine, other):
    zl = idx[0]
    for q in range(2):
        to = slice(q * 1024, q * 1024 + 1024)
        for out, z in ((mine, zl), (other, 1 - zl)):
            cols = pl.ds(pl.multiple_of(q * 2048 + z * 1024, 1024), 1024)
            out[:, to] = w[:, cols].astype(bf16)


def halves_kernel(mine, got, e0, e1):
    for z, w in enumerate((mine, got)):
        e0[z] = w[:, :CUT]
        e1[z] = w[:, CUT:]


def out_kernel(*refs):
    idx = refs[0]
    own, three, two = refs[1:5], refs[5], refs[6]
    part = (three[0], three[1], two[...], three[2])
    ya, xa = refs[7:11], refs[11:15]
    keep, send, att, acc0, acc1 = refs[15:20]
    zl, zh, c = idx[0], idx[3], idx[4]
    for s in range(4):
        k = (zh + 4 - s) % 4
        rows = pl.ds(pl.multiple_of(k % 2 * ROWS, ROWS), ROWS)
        att[k // 2 * 2 + c, rows] = own[s][...]
        att[k // 2 * 2 + 1 - c, rows] = part[s]
    nt = (((1,), (1,)), ((), ()))

    def add(a, acc, first):
        def step(t, carry):
            for u in range(2):
                cols = pl.ds(pl.multiple_of(t * 512 + u * 256, 256), 256)
                lhs = jnp.concatenate([r[:, :, :, cols].reshape(-1, 256) for r in a], axis=0)
                rhs = att[first + t][:, u * 256 : u * 256 + 256]
                acc[...] += lax.dot_general(lhs, rhs, nt, preferred_element_type=f32)
            return carry

        return step

    acc0[...] = jnp.zeros((1024, 256), f32)
    acc1[...] = jnp.zeros((1024, 256), f32)
    for a, acc, first, last in ((ya, acc0, 0, CUT), (xa, acc1, CUT, 2048)):
        lax.fori_loop(0, (last - first) // 512, add(a, acc, first // 512), 0)
    here = pl.ds(pl.multiple_of(zl * ROWS, ROWS), ROWS)
    there = pl.ds(pl.multiple_of(ROWS - zl * ROWS, ROWS), ROWS)
    for xs in range(4):
        for ys in range(4):
            i, j = (ys * 4 + xs) * 64, (xs * 4 + ys) * 64
            keep[xs, ys] = acc0[i : i + 64, here] + acc1[j : j + 64, here]
            total = (acc0[i : i + 64, there] + acc1[j : j + 64, there]).astype(bf16)
            send[xs, ys, 0:32] = total[32:]
            send[xs, ys, 32:64] = total[:32]


def add_kernel(keep, got, low, up):
    for xs in range(2):
        low[xs] = (keep[xs] + got[xs].astype(f32)).astype(bf16)
        up[xs] = (keep[xs + 2] + got[xs + 2].astype(f32)).astype(bf16)


def final_kernel(*refs):
    idx = refs[0]
    own = refs[1:9]
    part = [refs[9][i] for i in range(4)] + [refs[10][i] for i in range(2)] + [refs[11][...], refs[12][...]]
    hid, gain, new, normed, pieces, res = refs[13:19]
    zl, x, y, zh, c = (idx[i] for i in range(5))
    where = ((0, 0), (0, 1), (1, 0), (3, 1), (1, 1), (3, 0), (2, 0), (2, 1))
    for i, (s, h) in enumerate(where):
        t = ((zh + 4 - s) % 4) * 2
        pieces[t + c, 2 * h : 2 * h + 2] = own[i][...]
        pieces[t + 1 - c, 2 * h : 2 * h + 2] = part[i]
    a = lax.broadcasted_iota(jnp.int32, (ROWS, ROWS), 0)
    b = lax.broadcasted_iota(jnp.int32, (ROWS, ROWS), 1)
    eye = jnp.where(a == b, 1.0, 0.0).astype(bf16)
    nt = (((1,), (1,)), ((), ()))

    def step(j, total):
        xs, ys = j // 4, j % 4
        for zs in range(2):
            dp = ((zl ^ zs) * 4 + (x + 4 - xs) % 4) * 4 + (y + 4 - ys) % 4
            cols = pl.ds(pl.multiple_of(dp * 256, 256), 256)
            chunk = jnp.concatenate(
                [pieces[t, xs, ys, zs * 32 : zs * 32 + 32] for t in range(8)], axis=0
            )
            mixed = lax.dot_general(eye, chunk, nt, preferred_element_type=f32)
            r = hid[:, cols].astype(f32) + mixed
            total = total + r * r
            res[:, cols] = r
            new[:, cols] = r.astype(bf16)
        return total

    total = lax.fori_loop(0, 16, step, jnp.zeros((ROWS, 256), f32), unroll=2)
    scale = lax.rsqrt(jnp.sum(total, axis=-1, keepdims=True) / D + epsilon)

    def finish(j, carry):
        cols = pl.ds(pl.multiple_of(j * 1024, 1024), 1024)
        normed[:, cols] = (res[:, cols] * scale * gain[:, cols]).astype(bf16)
        return carry

    lax.fori_loop(0, 8, finish, 0)


def call(kernel, outs, *args, scratch=(), limit=16, near=True):
    def scalars(a):
        return a.dtype == jnp.int32 and a.ndim == 1

    return pl.pallas_call(
        kernel,
        out_shape=outs,
        in_specs=[SM if scalars(a) else VM for a in args],
        out_specs=jax.tree.map(lambda _: VM, outs),
        scratch_shapes=[pltpu.VMEM(*x) for x in scratch],
        compiler_params=pltpu.CompilerParams(vmem_limit_bytes=limit << 20),
    )(*[a if scalars(a) or not near else pltpu.with_memory_space_constraint(a, pltpu.VMEM) for a in args])


def fetch_kernel(keys, vals, keys_out, vals_out, sems):
    first = pltpu.make_async_copy(keys, keys_out, sems.at[0])
    second = pltpu.make_async_copy(vals, vals_out, sems.at[1])
    first.start()
    second.start()
    first.wait()
    second.wait()


def fetch(keys, vals):
    cache = pltpu.VMEM((ROWS, 64, HEAD_DIM), bf16)
    hbm = pl.BlockSpec(memory_space=pl.ANY)
    return pl.pallas_call(
        fetch_kernel,
        out_shape=[cache, cache],
        in_specs=[hbm, hbm],
        out_specs=[VM, VM],
        scratch_shapes=[pltpu.SemaphoreType.DMA((2,))],
        compiler_params=pltpu.CompilerParams(vmem_limit_bytes=1 << 20),
        name="fetch",
    )(keys, vals)


def body(hidden, q_weight, k_weight, v_weight, o_weight, input_gain, post_gain, key_cache, value_cache, lengths):
    zl, x, y, zh, c = (lax.axis_index(a) for a in ("zl", "x", "y", "zh", "c"))
    idx = idx0 = jnp.stack([zl, x, y, zh, c]).astype(jnp.int32)
    sds, vm = jax.ShapeDtypeStruct, pltpu.VMEM

    def move(value, axis, step):
        return shift(value, axis, 2 if axis in ("zl", "c") else 4, step)

    cut = call(cut_kernel, vm((8, 32, 768), bf16), q_weight, k_weight, v_weight, near=False, limit=60)
    block = lax.all_to_all(cut, ("zh", "c"), split_axis=0, concat_axis=0, tiled=True)
    block = block.reshape(256, 768)
    across = move(block, "zl", 1)
    w1, w3 = move(block, "x", 1), move(block, "x", 3)
    v1, v3 = move(across, "x", 1), move(across, "x", 3)
    wa, wb = move(w1[:128], "x", 1), move(w3[128:], "x", 3)
    va, vb = move(v1[:128], "x", 1), move(v3[128:], "x", 3)

    half = pltpu.HBM((64, 2048), bf16)
    h0, *hs = call(
        norm_kernel,
        [pltpu.HBM((2, 64, 2048), bf16), half, half, half],
        idx, hidden, input_gain.reshape(1, D),
        scratch=[((ROWS, 128), f32)],
    )
    hown = [move(hs[s - 1], "y", s) for s in (1, 2, 3)]
    hpart = move(jnp.stack(hown), "c", 1)

    acc = call(first_kernel, vm((512, 768), f32), h0, *hown, hpart, block, w1, w3, across, limit=8)
    full, short = vm((ROWS, 768), f32), vm((ROWS, 768), bf16)
    parts = call(second_kernel, [full, short, short, short], h0, *hown, hpart, v1, v3, wa, wb, va, vb, acc, limit=8)
    back = [move(parts[s], "y", -s) for s in (1, 2, 3)]

    index_row = jnp.arange(64, dtype=f32)
    frequency = jnp.exp(-math.log(rope_base) * index_row / 64)
    angle = lengths.astype(f32)[:, None] * frequency[None, :]
    cos, sin = jnp.cos(angle), jnp.sin(angle)
    head = sds((ROWS, 128), bf16)
    attended, fresh, newv = call(
        attend_kernel,
        [vm((ROWS, 512), bf16), head, head],
        idx, parts[0], *back,
        jnp.concatenate([cos, cos], axis=1),
        jnp.concatenate([-sin, sin], axis=1),
        jnp.broadcast_to(lengths.astype(f32)[:, None], (ROWS, 128)),
        *fetch(key_cache.reshape(ROWS, 64, 128), value_cache.reshape(ROWS, 64, 128)),
        scratch=[
            ((ROWS, 768), f32),
            ((16, 4, 8, 128), f32),
            ((16, 8, 128), f32),
            ((16, 8, 128), f32),
            ((16, 32, 512), f32),
            ((16, 8, 512), f32),
        ],
    )

    shard = vm((32, 2048), bf16)
    mine_o, other_o = call(rows_kernel, [shard] * 2, idx0, o_weight, near=False, limit=60)
    e0, e1 = call(
        halves_kernel,
        [vm((2, 32, CUT), bf16), vm((2, 32, 2048 - CUT), bf16)],
        mine_o, move(other_o, "zl", 1),
    )
    around = [e0] + [move(e0, "x", s) for s in (1, 2, 3)]
    s0 = jnp.stack(around)
    s1 = jnp.stack([e1] + [move(e1, "y", s) for s in (1, 2, 3)])
    rows_y = [s0] + [move(s0, "y", s) for s in (1, 2, 3)]
    rows_x = [s1] + [move(s1, "x", s) for s in (1, 2, 3)]

    def deal_heads(value, turn):
        pairs = []
        for z in range(8):
            to = z // 2 % 2 * 4 + (z % 2 + z // 4 * 2 + turn) % 4
            pairs.append((z % 2 * 4 + z // 2, to))
        return lax.ppermute(value, ("zl", "zh"), pairs)

    def spread(own):
        first = move(jnp.stack([own[0], own[1], own[3]]), "c", 1)
        return own + [first, move(own[2], "c", 1)]

    heads = spread([deal_heads(attended, s) for s in range(4)])
    tile = (4, 4, 64, ROWS)
    keep, send = call(
        out_kernel,
        [vm(tile, f32), vm(tile, bf16)],
        idx, *heads, *rows_y, *rows_x,
        scratch=[((4, 256, 512), bf16), ((1024, 256), f32), ((1024, 256), f32)],
    )
    half_tile = vm((2, 4, 64, ROWS), bf16)
    low, up = call(add_kernel, [half_tile] * 2, keep, move(send, "zl", 1), limit=4)
    a1, a3 = move(low, "zh", 1), move(up, "zh", 3)
    b1, b3 = move(up, "zh", 1), move(low, "zh", 3)
    f1, f3 = move(a1, "zh", 1), move(a3, "zh", 3)
    pieces = [low, up, a1, a3, b1, b3, f1, f3]
    pieces += [move(jnp.stack([low, up, a1, a3]), "c", 1), move(jnp.stack([b1, b3]), "c", 1)]
    pieces += [move(f1, "c", 1), move(f3, "c", 1)]
    new_hidden, normed = call(
        final_kernel,
        [sds((ROWS, D), bf16)] * 2,
        idx, *pieces, hidden, post_gain.reshape(1, D),
        scratch=[((8, 4, 4, 64, ROWS), bf16), ((ROWS, D), f32)],
    )
    return (new_hidden, normed, fresh.reshape(ROWS, 1, 128), newv.reshape(ROWS, 1, 128))


def solution(mesh):
    torus = Mesh(mesh.devices.reshape(2, 4, 4, 4, 2), ("zl", "x", "y", "zh", "c"))
    dp, tensor = ("zl", "x", "y"), ("zh", "c")
    in_specs = (
        P(dp, None),
        P(dp + tensor, None),
        P(dp + tensor, None),
        P(dp + tensor, None),
        P(dp + tensor, None),
        P(),
        P(),
        P(dp, None, tensor, None),
        P(dp, None, tensor, None),
        P(dp),
    )
    out_specs = (P(dp, None), P(dp, None), P(dp, tensor, None), P(dp, tensor, None))
    return jax.shard_map(body, mesh=torus, in_specs=in_specs, out_specs=out_specs, check_vma=False)
```
